32 devices in a mesh: sweep: 2 (over x), expert: 4 (over y, core), fsdp: 4 (over z).
Axes of the slice: x: 2, y: 2, z: 4, core: 2. Of those that a mesh axis runs over, the one named last changes fastest.
Arguments:
- tokens: bfloat16 [4096, 2048], P(('sweep', 'expert', 'fsdp')), parts along dimension 0, may hold values from -6 to 6
- context: bfloat16 [4096, 2048], P(('sweep', 'expert', 'fsdp')), parts along dimension 0, may hold values from -6 to 6
- out_proj: bfloat16 [4096, 2048], P(('sweep', 'expert', 'fsdp')), parts along dimension 0, may hold values from -0.125 to 0.125
- norm_gain: float32 [4096], P('sweep'), parts along dimension 0, may hold values from 0.1 to 1.9
- router: bfloat16 [4096, 8], P('sweep'), parts along dimension 0, may hold values from -0.125 to 0.125
- expert_ids: int32 [4096, 2], P(('sweep', 'expert', 'fsdp')), parts along dimension 0, may hold values from 0 to 7, all different within a row; in each aligned block of 128 rows (0 to 127, 128 to 255, ...) at most 40 rows name the same one
- w_gate_up: bfloat16 [32, 2, 704, 2048], P(('sweep', 'expert', 'fsdp')), parts along dimension 0, may hold values from -0.125 to 0.125
- w_down: bfloat16 [32, 704, 2048], P(('sweep', 'expert', 'fsdp')), parts along dimension 0, may hold values from -0.15625 to 0.15625
Outputs:
- layer_out: bfloat16 [4096, 2048], P(('sweep', 'expert', 'fsdp')), parts along dimension 0
The draws below stay inside these ranges and needn't reach their ends.
There are 2 independent parts, one for each index of `sweep`. The reference program is written for one: setup_inputs(seed, part) draws one part's arguments, and reference() takes and returns one part's arrays. A program takes and returns all parts, laid end to end along the dimension named above; each array names one. Nothing has to cross between parts.
Inputs may be any that keep to these rules, and one draw needn't show every extreme that they name: `expert_ids`: each row names two different experts. Among the rows of one device no expert is named more than 40 times, a bound that some block reaches.
All inputs are finite; a program needn't handle non-finite values.
Results may differ from the reference program's by a relative error of at most 0.012.
Values may be sent and summed in bfloat16 or wider, within the bound.
A program may use at most 64 MiB of HBM per device.

```python
import math
import jax
import jax.numpy as jnp
import numpy as np
from jax import lax

D = 2048
FF = 1408
EXPERTS = 8
TOK_DEV = 128
CAP = 40
TOKENS = 2048
N_EXPERT = 4
N_FSDP = 4


def block_scale(own_key, dims, cuts, least, high):
    def one(dim, blocks):
        steps = jax.random.uniform(jax.random.fold_in(jax.random.fold_in(own_key, 6), dim), (blocks,), jnp.float32, least / len(cuts), high / len(cuts))
        return jnp.repeat(jnp.exp(steps), dims[dim] // blocks).reshape((-1,) + (1,) * (len(dims) - dim - 1))

    factor_of = one(*cuts[0])
    for cut in cuts[1:]:
        factor_of = factor_of * one(*cut)
    return factor_of


def assign_block(own_key, own, number, rows, number_of, top, most, skew):
    order = jax.random.permutation(own_key, number_of)
    packed, ordinary = portions_of(number_of, rows * top, most, skew, True), portions_of(number_of, rows * top, most, skew, False)
    places = jnp.arange(number_of)

    def named(lengths, turn):
        used = int((lengths > 0).sum())
        fixed = max(1, used // 4)
        moved = fixed + (places - fixed + turn * (used - fixed)) % max(1, number_of - fixed)
        return jnp.zeros((number_of,), jnp.int32).at[order[jnp.where(places < fixed, places, moved)]].set(jnp.asarray(lengths, jnp.int32))

    lengths = jnp.where(number % 4 == 0, named(packed, number // 4), named(ordinary, number - number // 4 - 1))
    mixed = jax.random.permutation(jax.random.fold_in(own, 3), number_of)
    giver, receiver = mixed[0:number_of // 2 * 2:2], mixed[1:number_of // 2 * 2:2]
    margin = jnp.minimum(lengths[giver] - 1, most - lengths[receiver]) // 2
    margin = jnp.where((giver == order[0]) | (receiver == order[0]) | (lengths[receiver] == 0), 0, jnp.maximum(margin, 0))
    moved = jax.random.randint(jax.random.fold_in(own, 4), (number_of // 2,), 0, 1 << 20) % (margin + 1)
    lengths = lengths.at[giver].add(-moved).at[receiver].add(moved)
    items = jnp.searchsorted(jnp.cumsum(lengths), jnp.arange(rows * top), side="right").astype(jnp.int32)
    listing = items.reshape(top, rows).T
    listing = listing[jax.random.permutation(jax.random.fold_in(own, 1), rows)]
    turn = jax.random.randint(jax.random.fold_in(own, 2), (rows, 1), 0, top)
    return jnp.take_along_axis(listing, (jnp.arange(top)[None, :] + turn) % top, axis=1)


def portions_of(count, total, limit, skew, full):
    weights = [(1 << 20) // math.isqrt(standing ** skew) + 1 for standing in range(1, count + 1)]
    largest = limit if full else min(limit, max(-(-total // count), total * weights[0] // sum(weights)))
    least = 1 if total - largest >= count - 1 else 0
    counts, spare = [largest] + [least] * (count - 1), total - largest - least * (count - 1)
    while spare > 0:
        movable = [i for i in range(1, count) if counts[i] < largest] or [i for i in range(1, count) if counts[i] < limit]
        mass, left = sum([weights[i] for i in movable]), spare
        for i in movable:
            more = min(limit - counts[i], max(1, left * weights[i] // mass), spare)
            counts[i] = counts[i] + more
            spare = spare - more
    return np.array(counts)


def scatter_about(rng, shape, scale, most, split=(), held_as=jnp.bfloat16):
    entries = scale * jax.random.normal(rng, shape, jnp.float32)
    if split:
        entries = entries * block_scale(rng, shape, split, -0.22, 0.18)
    return jnp.clip(entries, -most, most).astype(held_as)


def setup_inputs(seed: int = 0, part: int = 0) -> dict:
    keys = jax.random.split(jax.random.key(seed), 9)
    part_keys = jax.random.split(jax.random.fold_in(keys[8], part), 9)
    tokens = scatter_about(part_keys[0], (TOKENS, D), 1.0, 6.0, ((0, 16),))
    context = scatter_about(part_keys[1], (TOKENS, D), 1.0, 6.0, ((0, 16),))
    out_proj = scatter_about(part_keys[2], (D, D), D ** -0.5, 0.125, ((0, 16),))
    norm_gain = jnp.clip(1.0 + 0.18 * jax.random.normal(part_keys[3], (D,), jnp.float32), 0.1, 1.9)
    router = scatter_about(part_keys[4], (D, EXPERTS), D ** -0.5, 0.125)
    expert_ids_keys = jax.random.split(jax.random.fold_in(part_keys[5], 1), TOKENS // TOK_DEV)
    expert_ids_turns = jax.random.permutation(jax.random.fold_in(part_keys[5], 3), TOKENS // TOK_DEV)
    expert_ids = jax.vmap(lambda own, number: assign_block(jax.random.fold_in(part_keys[5], 2), own, number, TOK_DEV, EXPERTS, 2, CAP, 2))(expert_ids_keys, expert_ids_turns).reshape((TOKENS, 2))
    w_gate_up = scatter_about(part_keys[6], (2 * EXPERTS, 2, FF // 2, D), D ** -0.5, 0.125, ((0, 16),))
    w_down = scatter_about(part_keys[7], (2 * EXPERTS, FF // 2, D), FF ** -0.5, 0.15625, ((0, 16),))
    return dict(tokens=tokens, context=context, out_proj=out_proj, norm_gain=norm_gain, router=router, expert_ids=expert_ids, w_gate_up=w_gate_up, w_down=w_down)


def reference(tokens, context, out_proj, norm_gain, router, expert_ids, w_gate_up, w_down):
    attended = jnp.dot(context, out_proj, preferred_element_type=jnp.float32)
    residual_in = (tokens.astype(jnp.float32) + attended).astype(jnp.bfloat16)
    widened = residual_in.astype(jnp.float32)
    inv_rms = lax.rsqrt(lax.optimization_barrier(jnp.mean(widened * widened, axis=1, keepdims=True)) + 1e-05)
    normed = (widened * inv_rms * norm_gain).astype(jnp.bfloat16)
    logits = jnp.dot(normed, router, preferred_element_type=jnp.float32)
    picked = jnp.take_along_axis(logits, expert_ids, axis=1)
    scores = jax.nn.sigmoid(picked)
    gate_vals = scores / lax.optimization_barrier(jnp.sum(scores, axis=1, keepdims=True))
    experts = EXPERTS
    blocks = N_EXPERT * N_FSDP
    ids_block = expert_ids.reshape(blocks, 2 * TOK_DEV)
    onehot = (ids_block[:, :, None] == jnp.arange(experts, dtype=jnp.int32)[None, None, :]).astype(jnp.int32)
    before = jnp.cumsum(onehot, axis=1) - onehot
    places = lax.optimization_barrier(jnp.sum(before * onehot, axis=2))
    block_of = jnp.arange(blocks, dtype=jnp.int32)[:, None]
    slot_index = ((ids_block * blocks + block_of) * CAP + places).reshape(-1).astype(jnp.int32)
    assign = jnp.arange(2 * TOKENS, dtype=jnp.int32)
    table_tok = jnp.full((experts * blocks * CAP,), TOKENS, jnp.int32).at[slot_index].set(assign // 2)
    table_gate = jnp.zeros((experts * blocks * CAP,), jnp.float32).at[slot_index].set(gate_vals.reshape(-1))
    padded = jnp.concatenate([normed, jnp.zeros((1, D), jnp.bfloat16)], axis=0)
    half_units = FF // 2

    def one_expert(running, inputs):
        slot_tokens, slot_gates, gate_up_w, down_w = inputs
        taken = padded[slot_tokens]
        total = jnp.zeros((taken.shape[0], D), jnp.float32)
        for half in range(2):
            gate_val = jnp.dot(taken, gate_up_w[half, 0].T, preferred_element_type=jnp.float32)
            up_val = jnp.dot(taken, gate_up_w[half, 1].T, preferred_element_type=jnp.float32)
            hidden = (jax.nn.silu(gate_val) * up_val).astype(jnp.bfloat16)
            piece = jnp.dot(hidden, down_w[half], preferred_element_type=jnp.float32).astype(jnp.bfloat16)
            piece = lax.optimization_barrier(piece)
            total = total + piece.astype(jnp.float32)
        combined = lax.optimization_barrier(total.astype(jnp.bfloat16)).astype(jnp.float32)
        running = running.at[slot_tokens].add(slot_gates[:, None] * combined)
        return (running, None)
    start_acc = jnp.zeros((TOKENS + 1, D), jnp.float32)
    running, unused = lax.scan(one_expert, start_acc, (table_tok.reshape(experts, -1), table_gate.reshape(experts, -1), w_gate_up.reshape(experts, 2, 2, half_units, D), w_down.reshape(experts, 2, half_units, D)))
    return (widened + running[:TOKENS]).astype(jnp.bfloat16)
```

```python
import functools

import jax
import jax.numpy as jnp
from jax import lax
from jax.experimental import pallas as pl
from jax.experimental.pallas import tpu as pltpu
from jax.sharding import PartitionSpec as P

eps_norm = 1e-05
MESH = pl.DeviceIdType.MESH
VMEM_GRANT = 60 * 1024 * 1024


def both(a, b):
    return jnp.logical_and(a, b)


def inside(i, n):
    return both(i >= 0, i < n)


def block_kernel(
    columns, members, cap, slots,
    tok, ctx, wout, gain, router, ids, gu_hbm, dn_hbm,
    out,
    gath, acc, gu, dn, outbox, inbox, part, partner, ret, resid,
    load_sem, ag_send, ag_recv, disp_send, disp_recv, fwd_send,
    part_send, part_recv, ret_send, ret_recv,
):
    n = columns * members
    lines = columns // 2
    pairs = members // 2
    experts = columns * pairs
    rows, width = tok.shape
    k_rows = wout.shape[0]
    my_e = lax.axis_index("expert")
    my_f = lax.axis_index("fsdp")
    me = my_e * members + my_f
    my_y, my_c = lax.div(my_e, 2), lax.rem(my_e, 2)
    my_p = lax.div(my_f, 2)
    my_expert = my_e * pairs + my_p

    def dev(e, f):
        return {"expert": e, "fsdp": f}

    load_gu = pltpu.make_async_copy(gu_hbm.at[0], gu, load_sem.at[0])
    load_dn = pltpu.make_async_copy(dn_hbm.at[0], dn, load_sem.at[1])
    load_gu.start()
    load_dn.start()

    barrier = pltpu.get_barrier_semaphore()

    def greet(i, _):
        other = lax.rem(me + i, n)
        pl.semaphore_signal(
            barrier, inc=1, device_id=dev(lax.div(other, members), lax.rem(other, members)),
            device_id_type=MESH)
        return 0

    lax.fori_loop(1, n, greet, 0)
    pl.semaphore_wait(barrier, n - 1)

    def place(e, f):
        return pl.ds(pl.multiple_of((e * members + f) * k_rows, k_rows), k_rows)

    def ag(e, f, way, target, own=False):
        b = e * members + f
        return pltpu.make_async_remote_copy(
            src_ref=wout if own else gath.at[place(e, f)],
            dst_ref=gath.at[place(e, f)],
            send_sem=ag_send.at[b, way],
            recv_sem=ag_recv.at[b],
            device_id=target,
            device_id_type=MESH)

    def ag_arrived(e, f):
        ag(e, f, 0, dev(my_y * 2 + 1 - my_c, my_f)).wait_recv()

    def z_copies(s, sign):
        fb, to = my_f + sign * s, my_f - sign
        k = 0 if sign == 1 else 1
        own = s == 0
        result = [(inside(to, members), lambda: ag(my_e, fb, k, dev(my_e, jnp.clip(to, 0, members - 1)), own))]
        if s > 0 or sign == 1:
            for j, ysign in enumerate((1, -1)):
                yt = my_y - ysign
                result.append((
                    inside(yt, lines),
                    lambda yt=yt, j=j: ag(my_e, fb, 2 + j, dev(jnp.clip(yt, 0, lines - 1) * 2 + my_c, my_f), own)))
            result.append((None, lambda: ag(my_e, fb, 4, dev(my_y * 2 + 1 - my_c, my_f), own)))
        return inside(fb, members), fb, result

    def y_copies(t, s, sign, ysign):
        fb = my_f + sign * s
        yb, yt = my_y + ysign * t, my_y - ysign
        e_b = yb * 2 + my_c
        j = 0 if ysign == 1 else 1
        result = []
        if t < lines - 1:
            result.append((
                inside(yt, lines),
                lambda: ag(e_b, fb, 2 + j, dev(jnp.clip(yt, 0, lines - 1) * 2 + my_c, my_f))))
        result.append((None, lambda: ag(e_b, fb, 4, dev(my_y * 2 + 1 - my_c, my_f))))
        return both(inside(fb, members), inside(yb, lines)), e_b, fb, result

    def apply(result, finish):
        for cond, make in result:
            def go(make=make):
                if finish:
                    make().wait_send()
                else:
                    make().start()
            if cond is None:
                go()
            else:
                pl.when(cond)(go)

    def z_step(s, finish=False):
        for sign in (1, -1):
            ok, fb, result = z_copies(s, sign)

            @pl.when(ok)
            def _():
                if s > 0 and not finish:
                    ag_arrived(my_e, fb)
                apply(result, finish)

    def y_step(t, s, finish=False):
        for ysign in (1, -1):
            for sign in (1, -1) if s else (1,):
                ok, e_b, fb, result = y_copies(t, s, sign, ysign)

                @pl.when(ok)
                def _():
                    if not finish:
                        ag_arrived(e_b, fb)
                    apply(result, finish)

    depth = members * k_rows
    col = min(512, width)

    def multiply(e):
        at = pl.ds(pl.multiple_of(e * depth, depth), depth)
        a = ctx[:, at]

        def one(i, _):
            cols = pl.ds(pl.multiple_of(i * col, col), col)
            acc[:, cols] += jnp.dot(a, gath[at, cols], preferred_element_type=jnp.float32)
            return 0

        lax.fori_loop(0, width // col, one, 0)

    z_step(0)
    gath[place(my_e, my_f), :] = wout[...]
    acc[...] = tok[...].astype(jnp.float32)
    for s in range(1, members):
        z_step(s)
        if lines > 1:
            y_step(1, s - 1)
    multiply(my_e)
    if lines > 1:
        y_step(1, members - 1)
        for t in range(2, lines):
            for s in range(members):
                y_step(t, s)

    id0, id1 = ids[:, 0:1], ids[:, 1:2]
    named = lax.broadcasted_iota(jnp.int32, (rows, experts), 1)
    hot0 = jnp.where(named == id0, 1.0, 0.0)
    hot1 = jnp.where(named == id1, 1.0, 0.0)
    earlier = jnp.where(
        lax.broadcasted_iota(jnp.int32, (rows, rows), 1) < lax.broadcasted_iota(jnp.int32, (rows, rows), 0),
        1.0, 0.0).astype(jnp.bfloat16)
    before = jnp.dot(earlier, (hot0 + hot1).astype(jnp.bfloat16), preferred_element_type=jnp.float32)
    slot0 = id0 * slots + jnp.sum(before * hot0, axis=1, keepdims=True).astype(jnp.int32)
    slot1 = id1 * slots + jnp.sum(before * hot1, axis=1, keepdims=True).astype(jnp.int32)
    slot_no = lax.broadcasted_iota(jnp.int32, (rows, experts * slots), 1)
    at0, at1 = slot_no == slot0, slot_no == slot1
    send_mask = jnp.where(jnp.logical_or(at0, at1), 1.0, 0.0).astype(jnp.bfloat16)

    def other_lines(t, _):
        multiply(lax.rem(my_y + t, lines) * 2 + my_c)
        return 0

    lax.fori_loop(1, lines, other_lines, 0)

    def other_core(t, _):
        e = lax.rem(my_y + t, lines) * 2 + 1 - my_c

        def one(f, _):
            ag_arrived(e, f)
            return 0

        lax.fori_loop(0, members, one, 0)
        multiply(e)
        return 0

    lax.fori_loop(0, lines, other_core, 0)

    rounded = acc[...].astype(jnp.bfloat16)
    resid[...] = rounded
    widened = rounded.astype(jnp.float32)
    inv = lax.rsqrt(jnp.mean(widened * widened, axis=1, keepdims=True) + eps_norm)
    normed = (widened * inv * gain[...]).astype(jnp.bfloat16)
    boxes = lax.dot_general(
        send_mask, normed, (((0,), (0,)), ((), ())), preferred_element_type=jnp.float32
    ).astype(jnp.bfloat16)
    for e in range(experts):
        outbox[e] = boxes[e * slots:(e + 1) * slots]

    def near_of(f, p):
        return jnp.clip(f, 2 * p, 2 * p + 1)

    def dispatch(e, p):
        x = e * pairs + p
        return pltpu.make_async_remote_copy(
            src_ref=outbox.at[x], dst_ref=inbox.at[me],
            send_sem=disp_send.at[x], recv_sem=disp_recv.at[me],
            device_id=dev(e, near_of(my_f, p)), device_id_type=MESH)

    def each_target(finish):
        for q in range(1, pairs + 1):
            p = lax.rem(my_p + q, pairs)

            def one(i, _):
                e = lax.rem(my_e + i, columns)
                if finish:
                    dispatch(e, p).wait_send()
                else:
                    dispatch(e, p).start()
                return 0

            lax.fori_loop(0 if q < pairs else 1, columns, one, 0)

    each_target(False)
    inbox[me] = outbox[my_expert]

    far_f = 4 * my_p + 1 - my_f

    def forward(b):
        return pltpu.make_async_remote_copy(
            src_ref=inbox.at[b], dst_ref=inbox.at[b],
            send_sem=fwd_send.at[b], recv_sem=disp_recv.at[b],
            device_id=dev(my_e, far_f), device_id_type=MESH)

    def group_of(g):
        return lax.rem(2 * my_p + g, members)

    def i_am_near(fs):
        return near_of(fs, my_p) == my_f

    def box_of(fs, i):
        return lax.rem(my_e + i, columns) * members + fs

    def pass_on(g):
        fs = group_of(g)

        def one(i, _):
            b = box_of(fs, i)

            @pl.when(b != me)
            def _():
                forward(b).wait_recv()

            @pl.when(i_am_near(fs))
            def _():
                forward(b).start()
            return 0

        lax.fori_loop(0, columns, one, 0)

    def give(b):
        return pltpu.make_async_remote_copy(
            src_ref=part.at[b], dst_ref=partner.at[b],
            send_sem=part_send.at[b], recv_sem=part_recv.at[b],
            device_id=dev(my_e, far_f), device_id_type=MESH)

    def give_back(b):
        return pltpu.make_async_remote_copy(
            src_ref=part.at[b], dst_ref=ret.at[my_expert],
            send_sem=ret_send.at[b], recv_sem=ret_recv.at[my_expert],
            device_id=dev(lax.div(b, members), lax.rem(b, members)), device_id_type=MESH)

    nt = (((1,), (1,)), ((), ()))

    def expert(g):
        fs = group_of(g)
        x = jnp.concatenate([inbox[e * members + fs] for e in range(columns)], axis=0)
        gate = lax.dot_general(x, gu[0], nt, preferred_element_type=jnp.float32)
        up = lax.dot_general(x, gu[1], nt, preferred_element_type=jnp.float32)
        hidden = (gate / (1.0 + jnp.exp(-gate)) * up).astype(jnp.bfloat16)
        piece = jnp.dot(hidden, dn[...], preferred_element_type=jnp.float32).astype(jnp.bfloat16)
        for e in range(columns):
            part[e * members + fs] = piece[e * slots:(e + 1) * slots]

        @pl.when(jnp.logical_not(i_am_near(fs)))
        def _():
            def one(i, _):
                give(box_of(fs, i)).start()
                return 0

            lax.fori_loop(0, columns, one, 0)

    def finish_group(g):
        fs = group_of(g)

        @pl.when(i_am_near(fs))
        def _():
            def one(i, _):
                b = box_of(fs, i)
                give(b).wait_recv()
                part[b] = (part[b].astype(jnp.float32) + partner[b].astype(jnp.float32)).astype(jnp.bfloat16)

                @pl.when(b == me)
                def _():
                    ret[my_expert] = part[b]

                @pl.when(b != me)
                def _():
                    give_back(b).start()
                return 0

            lax.fori_loop(0, columns, one, 0)

    logits = jnp.dot(normed, router[...], preferred_element_type=jnp.float32)
    s0 = jax.nn.sigmoid(jnp.sum(logits * hot0, axis=1, keepdims=True))
    s1 = jax.nn.sigmoid(jnp.sum(logits * hot1, axis=1, keepdims=True))
    total = s0 + s1
    weights = jnp.where(at0, s0 / total, 0.0) + jnp.where(at1, s1 / total, 0.0)
    weights_high = weights.astype(jnp.bfloat16)
    weights_low = (weights - weights_high.astype(jnp.float32)).astype(jnp.bfloat16)

    load_gu.wait()
    load_dn.wait()

    pass_on(0)

    def step(g, _):
        @pl.when(g + 1 < members)
        def _():
            pass_on(g + 1)

        expert(g)

        @pl.when(g > 0)
        def _():
            finish_group(g - 1)
        return 0

    lax.fori_loop(0, members, step, 0)
    finish_group(members - 1)

    def came_back(x, _):
        @pl.when(x != my_expert)
        def _():
            pltpu.make_async_remote_copy(
                src_ref=ret.at[x], dst_ref=ret.at[x],
                send_sem=disp_send.at[x], recv_sem=ret_recv.at[x],
                device_id=dev(my_e, far_f), device_id_type=MESH).wait_recv()
        return 0

    lax.fori_loop(0, experts, came_back, 0)
    results = jnp.concatenate([ret[x] for x in range(experts)], axis=0)
    mixed = jnp.dot(weights_high, results, preferred_element_type=jnp.float32)
    mixed = mixed + jnp.dot(weights_low, results, preferred_element_type=jnp.float32)
    out[...] = (resid[...].astype(jnp.float32) + mixed).astype(jnp.bfloat16)

    for s in range(members):
        z_step(s, True)
        for t in range(1, lines):
            y_step(t, s, True)
    each_target(True)

    def drain(b, _):
        fs = lax.rem(b, members)
        mine = lax.div(b, members)

        @pl.when(i_am_near(fs))
        def _():
            forward(b).wait_send()

            @pl.when(b != me)
            def _():
                give_back(b).wait_send()

        @pl.when(jnp.logical_not(i_am_near(fs)))
        def _():
            give(b).wait_send()
        return 0

    lax.fori_loop(0, n, drain, 0)


def on_device(tokens, context, out_proj, norm_gain, router, expert_ids, w_gate_up, w_down):
    rows, width = tokens.shape
    columns = lax.axis_size("expert")
    members = lax.axis_size("fsdp")
    n = columns * members
    experts = n // 2
    cap = 5 * rows // (2 * experts)
    slots = -(-cap // 8) * 8
    units = w_down.shape[1]
    vmem = pl.BlockSpec(memory_space=pltpu.VMEM)
    far = pl.BlockSpec(memory_space=pl.ANY)
    bf = jnp.bfloat16
    dma = pltpu.SemaphoreType.DMA
    call = pl.pallas_call(
        functools.partial(block_kernel, columns, members, cap, slots),
        out_shape=jax.ShapeDtypeStruct((rows, width), bf),
        in_specs=[vmem] * 6 + [far] * 2,
        out_specs=vmem,
        scratch_shapes=[
            pltpu.VMEM((n * out_proj.shape[0], width), bf),
            pltpu.VMEM((rows, width), jnp.float32),
            pltpu.VMEM((2, units, width), bf),
            pltpu.VMEM((units, width), bf),
            pltpu.VMEM((experts, slots, width), bf),
            pltpu.VMEM((n, slots, width), bf),
            pltpu.VMEM((n, slots, width), bf),
            pltpu.VMEM((n, slots, width), bf),
            pltpu.VMEM((experts, slots, width), bf),
            pltpu.VMEM((rows, width), bf),
            dma((2,)), dma((n, 5)), dma((n,)), dma((experts,)), dma((n,)), dma((n,)),
            dma((n,)), dma((n,)), dma((n,)), dma((experts,)),
        ],
        compiler_params=pltpu.CompilerParams(
            collective_id=0, has_side_effects=True, vmem_limit_bytes=VMEM_GRANT),
    )
    return call(tokens, context, out_proj, norm_gain.reshape(1, width), router, expert_ids, w_gate_up, w_down)


def solution(mesh):
    group = ("sweep", "expert", "fsdp")
    return jax.shard_map(
        on_device,
        mesh=mesh,
        in_specs=(
            P(group, None), P(group, None), P(group, None), P("sweep"), P("sweep", None),
            P(group, None), P(group, None, None, None), P(group, None, None),
        ),
        out_specs=P(group, None),
        check_vma=False,
    )
```

```python
import functools

import jax
import jax.numpy as jnp
from jax import lax
from jax.experimental import pallas as pl
from jax.experimental.pallas import tpu as pltpu
from jax.sharding import PartitionSpec as P

eps_norm = 1e-05
MESH = pl.DeviceIdType.MESH
VMEM_GRANT = 60 * 1024 * 1024


def both(a, b):
    return jnp.logical_and(a, b)


def inside(i, n):
    return both(i >= 0, i < n)


def block_kernel(
    columns, members, cap, slots,
    tok, ctx, wout, gain, router, ids, gu_hbm, dn_hbm,
    out,
    gath, acc, gu, dn, outbox, inbox, part, partner, ret, resid,
    load_sem, ag_send, ag_recv, disp_send, disp_recv, fwd_send,
    part_send, part_recv, ret_send, ret_recv,
):
    n = columns * members
    lines = columns // 2
    pairs = members // 2
    experts = columns * pairs
    rows, width = tok.shape
    k_rows = wout.shape[0]
    my_e = lax.axis_index("expert")
    my_f = lax.axis_index("fsdp")
    me = my_e * members + my_f
    my_y, my_c = lax.div(my_e, 2), lax.rem(my_e, 2)
    my_p = lax.div(my_f, 2)
    my_expert = my_e * pairs + my_p

    def dev(e, f):
        return {"expert": e, "fsdp": f}

    load_gu = pltpu.make_async_copy(gu_hbm.at[0], gu, load_sem.at[0])
    load_dn = pltpu.make_async_copy(dn_hbm.at[0], dn, load_sem.at[1])
    load_gu.start()
    load_dn.start()

    barrier = pltpu.get_barrier_semaphore()

    def greet(i, _):
        other = lax.rem(me + i, n)
        pl.semaphore_signal(
            barrier, inc=1, device_id=dev(lax.div(other, members), lax.rem(other, members)),
            device_id_type=MESH)
        return 0

    lax.fori_loop(1, n, greet, 0)
    pl.semaphore_wait(barrier, n - 1)

    def place(e, f):
        return pl.ds(pl.multiple_of((e * members + f) * k_rows, k_rows), k_rows)

    def ag(e, f, way, target, own=False):
        b = e * members + f
        return pltpu.make_async_remote_copy(
            src_ref=wout if own else gath.at[place(e, f)],
            dst_ref=gath.at[place(e, f)],
            send_sem=ag_send.at[b, way],
            recv_sem=ag_recv.at[b],
            device_id=target,
            device_id_type=MESH)

    def ag_arrived(e, f):
        ag(e, f, 0, dev(my_y * 2 + 1 - my_c, my_f)).wait_recv()

    def z_copies(s, sign):
        fb, to = my_f + sign * s, my_f - sign
        k = 0 if sign == 1 else 1
        own = s == 0
        result = [(inside(to, members), lambda: ag(my_e, fb, k, dev(my_e, jnp.clip(to, 0, members - 1)), own))]
        if s > 0 or sign == 1:
            for j, ysign in enumerate((1, -1)):
                yt = my_y - ysign
                result.append((
                    inside(yt, lines),
                    lambda yt=yt, j=j: ag(my_e, fb, 2 + j, dev(jnp.clip(yt, 0, lines - 1) * 2 + my_c, my_f), own)))
            result.append((None, lambda: ag(my_e, fb, 4, dev(my_y * 2 + 1 - my_c, my_f), own)))
        return inside(fb, members), fb, result

    def y_copies(t, s, sign, ysign):
        fb = my_f + sign * s
        yb, yt = my_y + ysign * t, my_y - ysign
        e_b = yb * 2 + my_c
        j = 0 if ysign == 1 else 1
        result = []
        if t < lines - 1:
            result.append((
                inside(yt, lines),
                lambda: ag(e_b, fb, 2 + j, dev(jnp.clip(yt, 0, lines - 1) * 2 + my_c, my_f))))
        result.append((None, lambda: ag(e_b, fb, 4, dev(my_y * 2 + 1 - my_c, my_f))))
        return both(inside(fb, members), inside(yb, lines)), e_b, fb, result

    def apply(result, finish):
        for cond, make in result:
            def go(make=make):
                if finish:
                    make().wait_send()
                else:
                    make().start()
            if cond is None:
                go()
            else:
                pl.when(cond)(go)

    def z_step(s, finish=False):
        for sign in (1, -1):
            ok, fb, result = z_copies(s, sign)

            @pl.when(ok)
            def _():
                if s > 0 and not finish:
                    ag_arrived(my_e, fb)
                apply(result, finish)

    def y_step(t, s, finish=False):
        for ysign in (1, -1):
            for sign in (1, -1) if s else (1,):
                ok, e_b, fb, result = y_copies(t, s, sign, ysign)

                @pl.when(ok)
                def _():
                    if not finish:
                        ag_arrived(e_b, fb)
                    apply(result, finish)

    depth = members * k_rows
    col = min(512, width)

    def multiply(e):
        at = pl.ds(pl.multiple_of(e * depth, depth), depth)
        a = ctx[:, at]

        def one(i, _):
            cols = pl.ds(pl.multiple_of(i * col, col), col)
            acc[:, cols] += jnp.dot(a, gath[at, cols], preferred_element_type=jnp.float32)
            return 0

        lax.fori_loop(0, width // col, one, 0)

    z_step(0)
    gath[place(my_e, my_f), :] = wout[...]
    acc[...] = tok[...].astype(jnp.float32)
    for s in range(1, members):
        z_step(s)
        if lines > 1:
            y_step(1, s - 1)
    multiply(my_e)
    if lines > 1:
        y_step(1, members - 1)
        for t in range(2, lines):
            for s in range(members):
                y_step(t, s)

    id0, id1 = ids[:, 0:1], ids[:, 1:2]
    named = lax.broadcasted_iota(jnp.int32, (rows, experts), 1)
    hot0 = jnp.where(named == id0, 1.0, 0.0)
    hot1 = jnp.where(named == id1, 1.0, 0.0)
    earlier = jnp.where(
        lax.broadcasted_iota(jnp.int32, (rows, rows), 1) < lax.broadcasted_iota(jnp.int32, (rows, rows), 0),
        1.0, 0.0).astype(jnp.bfloat16)
    before = jnp.dot(earlier, (hot0 + hot1).astype(jnp.bfloat16), preferred_element_type=jnp.float32)
    slot0 = id0 * slots + jnp.sum(before * hot0, axis=1, keepdims=True).astype(jnp.int32)
    slot1 = id1 * slots + jnp.sum(before * hot1, axis=1, keepdims=True).astype(jnp.int32)
    slot_no = lax.broadcasted_iota(jnp.int32, (rows, experts * slots), 1)
    at0, at1 = slot_no == slot0, slot_no == slot1
    send_mask = jnp.where(jnp.logical_or(at0, at1), 1.0, 0.0).astype(jnp.bfloat16)

    def other_lines(t, _):
        multiply(lax.rem(my_y + t, lines) * 2 + my_c)
        return 0

    lax.fori_loop(1, lines, other_lines, 0)

    def other_core(t, _):
        e = lax.rem(my_y + t, lines) * 2 + 1 - my_c

        def one(f, _):
            ag_arrived(e, f)
            return 0

        lax.fori_loop(0, members, one, 0)
        multiply(e)
        return 0

    lax.fori_loop(0, lines, other_core, 0)

    rounded = acc[...].astype(jnp.bfloat16)
    resid[...] = rounded
    widened = rounded.astype(jnp.float32)
    inv = lax.rsqrt(jnp.mean(widened * widened, axis=1, keepdims=True) + eps_norm)
    normed = (widened * inv * gain[...]).astype(jnp.bfloat16)
    boxes = lax.dot_general(
        send_mask, normed, (((0,), (0,)), ((), ())), preferred_element_type=jnp.float32
    ).astype(jnp.bfloat16)
    for e in range(experts):
        outbox[e] = boxes[e * slots:(e + 1) * slots]

    def near_of(f, p):
        return jnp.clip(f, 2 * p, 2 * p + 1)

    def dispatch(e, p):
        x = e * pairs + p
        return pltpu.make_async_remote_copy(
            src_ref=outbox.at[x], dst_ref=inbox.at[me],
            send_sem=disp_send.at[x], recv_sem=disp_recv.at[me],
            device_id=dev(e, near_of(my_f, p)), device_id_type=MESH)

    def each_target(finish):
        for q in range(pairs):
            p = lax.rem(my_p + q, pairs)

            def one(i, _):
                e = lax.rem(my_e + i, columns)
                if finish:
                    dispatch(e, p).wait_send()
                else:
                    dispatch(e, p).start()
                return 0

            lax.fori_loop(0 if q else 1, columns, one, 0)

    each_target(False)
    inbox[me] = outbox[my_expert]

    far_f = 4 * my_p + 1 - my_f

    def forward(b):
        return pltpu.make_async_remote_copy(
            src_ref=inbox.at[b], dst_ref=inbox.at[b],
            send_sem=fwd_send.at[b], recv_sem=disp_recv.at[b],
            device_id=dev(my_e, far_f), device_id_type=MESH)

    upper = 4 * my_p >= members

    def group_of(g):
        k = jnp.where(g < 2, 1 - g, g)
        return lax.rem(jnp.where(upper, 2 * my_p + 1 - k, 2 * my_p + k) + members, members)

    def i_am_near(fs):
        return near_of(fs, my_p) == my_f

    def box_of(fs, i):
        return lax.rem(my_e + i, columns) * members + fs

    def pass_on(k):
        fs = jnp.where(lax.rem(my_f, 2) == 1, my_f + k, my_f - k)

        @pl.when(inside(fs, members))
        def _():
            def one(i, _):
                b = box_of(fs, i)

                @pl.when(b != me)
                def _():
                    forward(b).wait_recv()

                forward(b).start()
                return 0

            lax.fori_loop(0, columns, one, 0)

    def passed_here(fs):
        @pl.when(jnp.logical_not(i_am_near(fs)))
        def _():
            def one(i, _):
                forward(box_of(fs, i)).wait_recv()
                return 0

            lax.fori_loop(0, columns, one, 0)

    def give(b):
        return pltpu.make_async_remote_copy(
            src_ref=part.at[b], dst_ref=partner.at[b],
            send_sem=part_send.at[b], recv_sem=part_recv.at[b],
            device_id=dev(my_e, far_f), device_id_type=MESH)

    def give_back(b):
        return pltpu.make_async_remote_copy(
            src_ref=part.at[b], dst_ref=ret.at[my_expert],
            send_sem=ret_send.at[b], recv_sem=ret_recv.at[my_expert],
            device_id=dev(lax.div(b, members), lax.rem(b, members)), device_id_type=MESH)

    nt = (((1,), (1,)), ((), ()))

    def expert(g):
        fs = group_of(g)
        passed_here(fs)
        x = jnp.concatenate([inbox[e * members + fs] for e in range(columns)], axis=0)
        gate = lax.dot_general(x, gu[0], nt, preferred_element_type=jnp.float32)
        up = lax.dot_general(x, gu[1], nt, preferred_element_type=jnp.float32)
        hidden = (gate / (1.0 + jnp.exp(-gate)) * up).astype(jnp.bfloat16)
        piece = jnp.dot(hidden, dn[...], preferred_element_type=jnp.float32).astype(jnp.bfloat16)
        for e in range(columns):
            part[e * members + fs] = piece[e * slots:(e + 1) * slots]

        @pl.when(jnp.logical_not(i_am_near(fs)))
        def _():
            def one(i, _):
                give(box_of(fs, i)).start()
                return 0

            lax.fori_loop(0, columns, one, 0)

    def finish_group(g):
        fs = group_of(g)

        @pl.when(i_am_near(fs))
        def _():
            def one(i, _):
                b = box_of(fs, i)
                give(b).wait_recv()
                part[b] = (part[b].astype(jnp.float32) + partner[b].astype(jnp.float32)).astype(jnp.bfloat16)

                @pl.when(b == me)
                def _():
                    ret[my_expert] = part[b]

                @pl.when(b != me)
                def _():
                    give_back(b).start()
                return 0

            lax.fori_loop(0, columns, one, 0)

    logits = jnp.dot(normed, router[...], preferred_element_type=jnp.float32)
    s0 = jax.nn.sigmoid(jnp.sum(logits * hot0, axis=1, keepdims=True))
    s1 = jax.nn.sigmoid(jnp.sum(logits * hot1, axis=1, keepdims=True))
    total = s0 + s1
    weights = jnp.where(at0, s0 / total, 0.0) + jnp.where(at1, s1 / total, 0.0)
    weights_high = weights.astype(jnp.bfloat16)
    weights_low = (weights - weights_high.astype(jnp.float32)).astype(jnp.bfloat16)

    load_gu.wait()
    load_dn.wait()

    pass_on(0)

    def step(g, _):
        @pl.when(g + 1 < members)
        def _():
            pass_on(g + 1)

        expert(g)

        @pl.when(g > 0)
        def _():
            finish_group(g - 1)
        return 0

    lax.fori_loop(0, members, step, 0)
    finish_group(members - 1)

    def came_back(x, _):
        @pl.when(x != my_expert)
        def _():
            pltpu.make_async_remote_copy(
                src_ref=ret.at[x], dst_ref=ret.at[x],
                send_sem=disp_send.at[x], recv_sem=ret_recv.at[x],
                device_id=dev(my_e, far_f), device_id_type=MESH).wait_recv()
        return 0

    lax.fori_loop(0, experts, came_back, 0)
    results = jnp.concatenate([ret[x] for x in range(experts)], axis=0)
    mixed = jnp.dot(weights_high, results, preferred_element_type=jnp.float32)
    mixed = mixed + jnp.dot(weights_low, results, preferred_element_type=jnp.float32)
    out[...] = (resid[...].astype(jnp.float32) + mixed).astype(jnp.bfloat16)

    for s in range(members):
        z_step(s, True)
        for t in range(1, lines):
            y_step(t, s, True)
    each_target(True)

    def drain(b, _):
        fs = lax.rem(b, members)
        mine = lax.div(b, members)

        @pl.when(i_am_near(fs))
        def _():
            forward(b).wait_send()

            @pl.when(b != me)
            def _():
                give_back(b).wait_send()

        @pl.when(jnp.logical_not(i_am_near(fs)))
        def _():
            give(b).wait_send()
        return 0

    lax.fori_loop(0, n, drain, 0)


def on_device(tokens, context, out_proj, norm_gain, router, expert_ids, w_gate_up, w_down):
    rows, width = tokens.shape
    columns = lax.axis_size("expert")
    members = lax.axis_size("fsdp")
    n = columns * members
    experts = n // 2
    cap = 5 * rows // (2 * experts)
    slots = -(-cap // 8) * 8
    units = w_down.shape[1]
    vmem = pl.BlockSpec(memory_space=pltpu.VMEM)
    far = pl.BlockSpec(memory_space=pl.ANY)
    bf = jnp.bfloat16
    dma = pltpu.SemaphoreType.DMA
    call = pl.pallas_call(
        functools.partial(block_kernel, columns, members, cap, slots),
        out_shape=jax.ShapeDtypeStruct((rows, width), bf),
        in_specs=[vmem] * 6 + [far] * 2,
        out_specs=vmem,
        scratch_shapes=[
            pltpu.VMEM((n * out_proj.shape[0], width), bf),
            pltpu.VMEM((rows, width), jnp.float32),
            pltpu.VMEM((2, units, width), bf),
            pltpu.VMEM((units, width), bf),
            pltpu.VMEM((experts, slots, width), bf),
            pltpu.VMEM((n, slots, width), bf),
            pltpu.VMEM((n, slots, width), bf),
            pltpu.VMEM((n, slots, width), bf),
            pltpu.VMEM((experts, slots, width), bf),
            pltpu.VMEM((rows, width), bf),
            dma((2,)), dma((n, 5)), dma((n,)), dma((experts,)), dma((n,)), dma((n,)),
            dma((n,)), dma((n,)), dma((n,)), dma((experts,)),
        ],
        compiler_params=pltpu.CompilerParams(
            collective_id=0, has_side_effects=True, vmem_limit_bytes=VMEM_GRANT),
    )
    return call(tokens, context, out_proj, norm_gain.reshape(1, width), router, expert_ids, w_gate_up, w_down)


def solution(mesh):
    group = ("sweep", "expert", "fsdp")
    return jax.shard_map(
        on_device,
        mesh=mesh,
        in_specs=(
            P(group, None), P(group, None), P(group, None), P("sweep"), P("sweep", None),
            P(group, None), P(group, None, None, None), P(group, None, None),
        ),
        out_specs=P(group, None),
        check_vma=False,
    )
```

```python
import functools

import jax
import jax.numpy as jnp
from jax import lax
from jax.experimental import pallas as pl
from jax.experimental.pallas import tpu as pltpu
from jax.sharding import PartitionSpec as P

eps_norm = 1e-05
MESH = pl.DeviceIdType.MESH
VMEM_GRANT = 60 * 1024 * 1024


def both(a, b):
    return jnp.logical_and(a, b)


def inside(i, n):
    return both(i >= 0, i < n)


def block_kernel(
    columns, members, cap, slots,
    tok, ctx, wout, gain, router, ids, gu_hbm, dn_hbm,
    out,
    gath, acc, gu, dn, outbox, inbox, part, partner, ret, resid,
    load_sem, ag_send, ag_recv, disp_send, disp_recv, fwd_send,
    part_send, part_recv, ret_send, ret_recv,
):
    n = columns * members
    lines = columns // 2
    pairs = members // 2
    experts = columns * pairs
    rows, width = tok.shape
    k_rows = wout.shape[0]
    my_e = lax.axis_index("expert")
    my_f = lax.axis_index("fsdp")
    me = my_e * members + my_f
    my_y, my_c = lax.div(my_e, 2), lax.rem(my_e, 2)
    my_p = lax.div(my_f, 2)
    my_expert = my_e * pairs + my_p

    def dev(e, f):
        return {"expert": e, "fsdp": f}

    load_gu = pltpu.make_async_copy(gu_hbm.at[0], gu, load_sem.at[0])
    load_dn = pltpu.make_async_copy(dn_hbm.at[0], dn, load_sem.at[1])
    load_gu.start()
    load_dn.start()

    barrier = pltpu.get_barrier_semaphore()

    def greet(i, _):
        other = lax.rem(me + i, n)
        pl.semaphore_signal(
            barrier, inc=1, device_id=dev(lax.div(other, members), lax.rem(other, members)),
            device_id_type=MESH)
        return 0

    lax.fori_loop(1, n, greet, 0)
    pl.semaphore_wait(barrier, n - 1)

    def place(e, f):
        return pl.ds(pl.multiple_of((e * members + f) * k_rows, k_rows), k_rows)

    def ag(e, f, way, target, own=False):
        b = e * members + f
        return pltpu.make_async_remote_copy(
            src_ref=wout if own else gath.at[place(e, f)],
            dst_ref=gath.at[place(e, f)],
            send_sem=ag_send.at[b, way],
            recv_sem=ag_recv.at[b],
            device_id=target,
            device_id_type=MESH)

    def ag_arrived(e, f):
        ag(e, f, 0, dev(my_y * 2 + 1 - my_c, my_f)).wait_recv()

    def z_copies(s, sign):
        fb, to = my_f + sign * s, my_f - sign
        k = 0 if sign == 1 else 1
        own = s == 0
        result = [(inside(to, members), lambda: ag(my_e, fb, k, dev(my_e, jnp.clip(to, 0, members - 1)), own))]
        if s > 0 or sign == 1:
            for j, ysign in enumerate((1, -1)):
                yt = my_y - ysign
                result.append((
                    inside(yt, lines),
                    lambda yt=yt, j=j: ag(my_e, fb, 2 + j, dev(jnp.clip(yt, 0, lines - 1) * 2 + my_c, my_f), own)))
            result.append((None, lambda: ag(my_e, fb, 4, dev(my_y * 2 + 1 - my_c, my_f), own)))
        return inside(fb, members), fb, result

    def y_copies(t, s, sign, ysign):
        fb = my_f + sign * s
        yb, yt = my_y + ysign * t, my_y - ysign
        e_b = yb * 2 + my_c
        j = 0 if ysign == 1 else 1
        result = []
        if t < lines - 1:
            result.append((
                inside(yt, lines),
                lambda: ag(e_b, fb, 2 + j, dev(jnp.clip(yt, 0, lines - 1) * 2 + my_c, my_f))))
        result.append((None, lambda: ag(e_b, fb, 4, dev(my_y * 2 + 1 - my_c, my_f))))
        return both(inside(fb, members), inside(yb, lines)), e_b, fb, result

    def apply(result, finish):
        for cond, make in result:
            def go(make=make):
                if finish:
                    make().wait_send()
                else:
                    make().start()
            if cond is None:
                go()
            else:
                pl.when(cond)(go)

    def z_step(s, finish=False):
        for sign in (1, -1):
            ok, fb, result = z_copies(s, sign)

            @pl.when(ok)
            def _():
                if s > 0 and not finish:
                    ag_arrived(my_e, fb)
                apply(result, finish)

    def y_step(t, s, finish=False):
        for ysign in (1, -1):
            for sign in (1, -1) if s else (1,):
                ok, e_b, fb, result = y_copies(t, s, sign, ysign)

                @pl.when(ok)
                def _():
                    if not finish:
                        ag_arrived(e_b, fb)
                    apply(result, finish)

    depth = members * k_rows
    col = min(512, width)

    def multiply(e):
        at = pl.ds(pl.multiple_of(e * depth, depth), depth)
        a = ctx[:, at]

        def one(i, _):
            cols = pl.ds(pl.multiple_of(i * col, col), col)
            acc[:, cols] += jnp.dot(a, gath[at, cols], preferred_element_type=jnp.float32)
            return 0

        lax.fori_loop(0, width // col, one, 0)

    z_step(0)
    gath[place(my_e, my_f), :] = wout[...]
    acc[...] = tok[...].astype(jnp.float32)
    for s in range(1, members):
        z_step(s)
        if lines > 1:
            y_step(1, s - 1)
    multiply(my_e)
    if lines > 1:
        y_step(1, members - 1)
        for t in range(2, lines):
            for s in range(members):
                y_step(t, s)

    diagonal = jnp.where(
        lax.broadcasted_iota(jnp.int32, (rows, rows), 0) == lax.broadcasted_iota(jnp.int32, (rows, rows), 1), 1.0, 0.0)
    named_ids = ids[...].astype(jnp.float32)
    id0 = jnp.sum(diagonal * named_ids[0:1], axis=1, keepdims=True).astype(jnp.int32)
    id1 = jnp.sum(diagonal * named_ids[1:2], axis=1, keepdims=True).astype(jnp.int32)
    named = lax.broadcasted_iota(jnp.int32, (rows, experts), 1)
    hot0 = jnp.where(named == id0, 1.0, 0.0)
    hot1 = jnp.where(named == id1, 1.0, 0.0)
    earlier = jnp.where(
        lax.broadcasted_iota(jnp.int32, (rows, rows), 1) < lax.broadcasted_iota(jnp.int32, (rows, rows), 0),
        1.0, 0.0).astype(jnp.bfloat16)
    before = jnp.dot(earlier, (hot0 + hot1).astype(jnp.bfloat16), preferred_element_type=jnp.float32)
    slot0 = id0 * slots + jnp.sum(before * hot0, axis=1, keepdims=True).astype(jnp.int32)
    slot1 = id1 * slots + jnp.sum(before * hot1, axis=1, keepdims=True).astype(jnp.int32)
    slot_no = lax.broadcasted_iota(jnp.int32, (rows, experts * slots), 1)
    at0, at1 = slot_no == slot0, slot_no == slot1
    send_mask = jnp.where(jnp.logical_or(at0, at1), 1.0, 0.0).astype(jnp.bfloat16)

    def other_lines(t, _):
        multiply(lax.rem(my_y + t, lines) * 2 + my_c)
        return 0

    lax.fori_loop(1, lines, other_lines, 0)

    def other_core(t, _):
        e = lax.rem(my_y + t, lines) * 2 + 1 - my_c

        def one(f, _):
            ag_arrived(e, f)
            return 0

        lax.fori_loop(0, members, one, 0)
        multiply(e)
        return 0

    lax.fori_loop(0, lines, other_core, 0)

    rounded = acc[...].astype(jnp.bfloat16)
    resid[...] = rounded
    widened = rounded.astype(jnp.float32)
    inv = lax.rsqrt(jnp.mean(widened * widened, axis=1, keepdims=True) + eps_norm)
    normed = (widened * inv * gain[...]).astype(jnp.bfloat16)
    boxes = lax.dot_general(
        send_mask, normed, (((0,), (0,)), ((), ())), preferred_element_type=jnp.float32
    ).astype(jnp.bfloat16)
    for e in range(experts):
        outbox[e] = boxes[e * slots:(e + 1) * slots]

    def near_of(f, p):
        return jnp.clip(f, 2 * p, 2 * p + 1)

    def dispatch(e, p):
        x = e * pairs + p
        return pltpu.make_async_remote_copy(
            src_ref=outbox.at[x], dst_ref=inbox.at[me],
            send_sem=disp_send.at[x], recv_sem=disp_recv.at[me],
            device_id=dev(e, near_of(my_f, p)), device_id_type=MESH)

    def each_target(finish):
        for q in range(pairs):
            p = lax.rem(my_p + q, pairs)

            def one(i, _):
                e = lax.rem(my_e + i, columns)
                if finish:
                    dispatch(e, p).wait_send()
                else:
                    dispatch(e, p).start()
                return 0

            lax.fori_loop(0 if q else 1, columns, one, 0)

    each_target(False)
    inbox[me] = outbox[my_expert]

    far_f = 4 * my_p + 1 - my_f

    def forward(b):
        return pltpu.make_async_remote_copy(
            src_ref=inbox.at[b], dst_ref=inbox.at[b],
            send_sem=fwd_send.at[b], recv_sem=disp_recv.at[b],
            device_id=dev(my_e, far_f), device_id_type=MESH)

    upper = 4 * my_p >= members

    def group_of(g):
        k = jnp.where(g < 2, 1 - g, g)
        return lax.rem(jnp.where(upper, 2 * my_p + 1 - k, 2 * my_p + k) + members, members)

    def i_am_near(fs):
        return near_of(fs, my_p) == my_f

    def box_of(fs, i):
        return lax.rem(my_e + i, columns) * members + fs

    def pass_on(k):
        fs = jnp.where(lax.rem(my_f, 2) == 1, my_f + k, my_f - k)

        @pl.when(inside(fs, members))
        def _():
            def one(i, _):
                b = box_of(fs, i)

                @pl.when(b != me)
                def _():
                    forward(b).wait_recv()

                forward(b).start()
                return 0

            lax.fori_loop(0, columns, one, 0)

    def passed_here(fs):
        @pl.when(jnp.logical_not(i_am_near(fs)))
        def _():
            def one(i, _):
                forward(box_of(fs, i)).wait_recv()
                return 0

            lax.fori_loop(0, columns, one, 0)

    def give(b):
        return pltpu.make_async_remote_copy(
            src_ref=part.at[b], dst_ref=partner.at[b],
            send_sem=part_send.at[b], recv_sem=part_recv.at[b],
            device_id=dev(my_e, far_f), device_id_type=MESH)

    def give_back(b):
        return pltpu.make_async_remote_copy(
            src_ref=part.at[b], dst_ref=ret.at[my_expert],
            send_sem=ret_send.at[b], recv_sem=ret_recv.at[my_expert],
            device_id=dev(lax.div(b, members), lax.rem(b, members)), device_id_type=MESH)

    nt = (((1,), (1,)), ((), ()))

    def expert(g):
        fs = group_of(g)
        passed_here(fs)
        x = jnp.concatenate([inbox[e * members + fs] for e in range(columns)], axis=0)
        gate = lax.dot_general(x, gu[0], nt, preferred_element_type=jnp.float32)
        up = lax.dot_general(x, gu[1], nt, preferred_element_type=jnp.float32)
        hidden = (gate / (1.0 + jnp.exp(-gate)) * up).astype(jnp.bfloat16)
        piece = jnp.dot(hidden, dn[...], preferred_element_type=jnp.float32).astype(jnp.bfloat16)
        for e in range(columns):
            part[e * members + fs] = piece[e * slots:(e + 1) * slots]

        @pl.when(jnp.logical_not(i_am_near(fs)))
        def _():
            def one(i, _):
                give(box_of(fs, i)).start()
                return 0

            lax.fori_loop(0, columns, one, 0)

    def finish_group(g):
        fs = group_of(g)

        @pl.when(i_am_near(fs))
        def _():
            def one(i, _):
                b = box_of(fs, i)
                give(b).wait_recv()
                part[b] = (part[b].astype(jnp.float32) + partner[b].astype(jnp.float32)).astype(jnp.bfloat16)

                @pl.when(b == me)
                def _():
                    ret[my_expert] = part[b]

                @pl.when(b != me)
                def _():
                    give_back(b).start()
                return 0

            lax.fori_loop(0, columns, one, 0)

    logits = lax.dot_general(normed, router[...], nt, preferred_element_type=jnp.float32)
    s0 = jax.nn.sigmoid(jnp.sum(logits * hot0, axis=1, keepdims=True))
    s1 = jax.nn.sigmoid(jnp.sum(logits * hot1, axis=1, keepdims=True))
    total = s0 + s1
    weights = jnp.where(at0, s0 / total, 0.0) + jnp.where(at1, s1 / total, 0.0)
    weights_high = weights.astype(jnp.bfloat16)
    weights_low = (weights - weights_high.astype(jnp.float32)).astype(jnp.bfloat16)

    load_gu.wait()
    load_dn.wait()

    pass_on(0)

    def step(g, _):
        @pl.when(g + 1 < members)
        def _():
            pass_on(g + 1)

        expert(g)

        @pl.when(g > 0)
        def _():
            finish_group(g - 1)
        return 0

    lax.fori_loop(0, members, step, 0)
    finish_group(members - 1)

    def came_back(x, _):
        @pl.when(x != my_expert)
        def _():
            pltpu.make_async_remote_copy(
                src_ref=ret.at[x], dst_ref=ret.at[x],
                send_sem=disp_send.at[x], recv_sem=ret_recv.at[x],
                device_id=dev(my_e, far_f), device_id_type=MESH).wait_recv()
        return 0

    lax.fori_loop(0, experts, came_back, 0)
    results = jnp.concatenate([ret[x] for x in range(experts)], axis=0)
    mixed = jnp.dot(weights_high, results, preferred_element_type=jnp.float32)
    mixed = mixed + jnp.dot(weights_low, results, preferred_element_type=jnp.float32)
    out[...] = (resid[...].astype(jnp.float32) + mixed).astype(jnp.bfloat16)

    for s in range(members):
        z_step(s, True)
        for t in range(1, lines):
            y_step(t, s, True)
    each_target(True)

    def drain(b, _):
        fs = lax.rem(b, members)
        mine = lax.div(b, members)

        @pl.when(i_am_near(fs))
        def _():
            forward(b).wait_send()

            @pl.when(b != me)
            def _():
                give_back(b).wait_send()

        @pl.when(jnp.logical_not(i_am_near(fs)))
        def _():
            give(b).wait_send()
        return 0

    lax.fori_loop(0, n, drain, 0)


def on_device(tokens, context, out_proj, norm_gain, router, expert_ids, w_gate_up, w_down):
    rows, width = tokens.shape
    columns = lax.axis_size("expert")
    members = lax.axis_size("fsdp")
    n = columns * members
    experts = n // 2
    cap = 5 * rows // (2 * experts)
    slots = -(-cap // 8) * 8
    units = w_down.shape[1]
    vmem = pl.BlockSpec(memory_space=pltpu.VMEM)
    far = pl.BlockSpec(memory_space=pl.ANY)
    bf = jnp.bfloat16
    dma = pltpu.SemaphoreType.DMA
    call = pl.pallas_call(
        functools.partial(block_kernel, columns, members, cap, slots),
        out_shape=jax.ShapeDtypeStruct((rows, width), bf),
        in_specs=[vmem] * 6 + [far] * 2,
        out_specs=vmem,
        scratch_shapes=[
            pltpu.VMEM((n * out_proj.shape[0], width), bf),
            pltpu.VMEM((rows, width), jnp.float32),
            pltpu.VMEM((2, units, width), bf),
            pltpu.VMEM((units, width), bf),
            pltpu.VMEM((experts, slots, width), bf),
            pltpu.VMEM((n, slots, width), bf),
            pltpu.VMEM((n, slots, width), bf),
            pltpu.VMEM((n, slots, width), bf),
            pltpu.VMEM((experts, slots, width), bf),
            pltpu.VMEM((rows, width), bf),
            dma((2,)), dma((n, 5)), dma((n,)), dma((experts,)), dma((n,)), dma((n,)),
            dma((n,)), dma((n,)), dma((n,)), dma((experts,)),
        ],
        compiler_params=pltpu.CompilerParams(
            collective_id=0, has_side_effects=True, vmem_limit_bytes=VMEM_GRANT),
    )
    return call(tokens, context, out_proj, norm_gain.reshape(1, width), router.T, expert_ids.T, w_gate_up, w_down)


def solution(mesh):
    group = ("sweep", "expert", "fsdp")
    return jax.shard_map(
        on_device,
        mesh=mesh,
        in_specs=(
            P(group, None), P(group, None), P(group, None), P("sweep"), P("sweep", None),
            P(group, None), P(group, None, None, None), P(group, None, None),
        ),
        out_specs=P(group, None),
        check_vma=False,
    )
```
